32 devices in a mesh: lat: 16 (over z, y, x), lev: 2 (over core).
Axes of the slice: x: 2, y: 2, z: 4, core: 2. Of those that a mesh axis runs over, the one named last changes fastest.
Arguments:
- fields: float32 [160, 3, 16, 2560], P('lat', None, 'lev'), may hold values from 0.1 to 5
- lat_fraction: float32 [160], P('lat'), may hold values from 0 to 1
- lon_fraction: float32 [160], P('lat'), may hold values from 0 to 1
- lon_shift: int32 [160], P('lat'), may hold values from 0 to 2559
- departure_row: int32 [160], P('lat'), may hold values from 1 to 157, as said below
- extents: int32 [16, 2], P('lat'), may hold values from 1 to 4
Outputs:
- advected: float32 [160, 3, 16, 2560], P('lat', None, 'lev')
The draws below stay inside these ranges and needn't reach their ends.
Inputs may be any that keep to these rules, and one draw needn't show every extreme that they name: departure_row[r] lies within 39 rows of r.
All inputs are finite; a program needn't handle non-finite values.
Results may differ from the reference program's by a relative error of at most 0.0003.
Values sent between devices are 32-bit elements; how exact they have to be, the bound alone decides.
No kernel may reach another device: no remote copies, remote signals or barrier semaphores. Data moves between devices by JAX's collectives and lax.ppermute only.
A program may use at most 128 MiB of HBM per device.

```python
import math
import jax
import jax.numpy as jnp
from jax import lax

ROWS = 10
LON = 2560
FIELDS = 3
REACH = 4
NLAT = 160
LEV = 16
BANDS = 16


def band_phase(key):
    return jax.random.randint(jax.random.fold_in(key, 911), (), 0, 8 * ROWS)


def draw_fields(key, part):
    row_phase = band_phase(key)
    shifted_rows = (jnp.arange(NLAT, dtype=jnp.int32) + row_phase) % (8 * ROWS)
    row_angle = 2.0 * math.pi * shifted_rows.astype(jnp.float32) / (8 * ROWS)
    full_shape = (NLAT, FIELDS, LEV, LON)
    gain_row = jnp.exp(-0.5 * jnp.sin(row_angle))
    rough_part = jax.random.uniform(jax.random.fold_in(key, 23), full_shape, jnp.float32, 0.5, 2.0)
    return (gain_row[:, None, None, None] * rough_part).astype(jnp.float32)


def draw_departure_row(key, part):
    row_phase = band_phase(key)
    row_ids = jnp.arange(NLAT, dtype=jnp.int32)
    shifted_rows = (row_ids + row_phase) % (8 * ROWS)
    row_drift = jnp.clip(2 * (2 * ROWS - jnp.abs(shifted_rows - 4 * ROWS)), -2 * ROWS, 2 * ROWS)
    row_noise = jax.random.randint(jax.random.fold_in(key, 17), (NLAT,), -2 * ROWS, 2 * ROWS + 1)
    offsets = jnp.clip(row_drift + row_noise, -REACH * ROWS + 1, REACH * ROWS - 2)
    spread = jax.random.randint(jax.random.fold_in(key, 29), (NLAT,), 0, 1 << 20)
    north_offset = -(1 + spread % (REACH * ROWS - 1))
    south_offset = 1 + spread % (REACH * ROWS - 2)
    position = row_ids % ROWS
    offsets = jnp.where(position == 0, north_offset, offsets)
    offsets = jnp.where(position == ROWS - 1, south_offset, offsets)
    return jnp.clip(row_ids + offsets, 1, NLAT - 3).astype(jnp.int32)


def plant(array, rng, low, largest):
    spot = [jax.random.randint(jax.random.fold_in(rng, axis), (), 0, length) for axis, length in enumerate(array.shape)]
    widest = array.shape.index(max(array.shape))
    next_to = spot[:widest] + [(spot[widest] + 1) % array.shape[widest]] + spot[widest + 1:]
    return array.at[tuple(spot)].set(low).at[tuple(next_to)].set(largest)


def level_of(stream_key, shape, pieces, smallest, high):
    def one(axis_at, blocks):
        heights = jax.random.uniform(jax.random.fold_in(jax.random.fold_in(stream_key, 6), axis_at), (blocks,), jnp.float32, smallest / len(pieces), high / len(pieces))
        return jnp.repeat(jnp.exp(heights), shape[axis_at] // blocks).reshape((-1,) + (1,) * (len(shape) - axis_at - 1))

    gain = one(*pieces[0])
    for cut in pieces[1:]:
        gain = gain * one(*cut)
    return gain


def setup_inputs(seed: int = 0) -> dict:
    key_of = jax.random.split(jax.random.key(seed), 7)
    return {
        "fields": draw_fields(jax.random.fold_in(key_of[6], 71), 0),
        "lat_fraction": jnp.clip(1.0 * jax.random.uniform(key_of[1], (NLAT,), jnp.float32) ** level_of(key_of[1], (NLAT,), ((0, 16),), -0.2, 0.2), 0.0, 1.0),
        "lon_fraction": jnp.clip(1.0 * jax.random.uniform(key_of[2], (NLAT,), jnp.float32) ** level_of(key_of[2], (NLAT,), ((0, 16),), -0.2, 0.2), 0.0, 1.0),
        "lon_shift": plant(jax.random.randint(key_of[3], (NLAT,), 0, LON), jax.random.fold_in(key_of[3], 1), 0, LON - 1).astype(jnp.int32),
        "departure_row": draw_departure_row(jax.random.fold_in(key_of[6], 71), 0),
        "extents": plant(jax.random.randint(key_of[5], (BANDS, 2), 1, REACH + 1), jax.random.fold_in(key_of[5], 1), 1, REACH).astype(jnp.int32),
    }


def cubic_weights(fraction):
    return jnp.stack([-fraction * (fraction - 1.0) * (fraction - 2.0) / 6.0,
                      (fraction + 1.0) * (fraction - 1.0) * (fraction - 2.0) / 2.0,
                      -(fraction + 1.0) * fraction * (fraction - 2.0) / 2.0,
                      (fraction + 1.0) * fraction * (fraction - 1.0) / 6.0])


def along_lon(column, lon_w, shift_value):
    lon_count = column.shape[-1]
    doubled = jnp.concatenate([column, column], axis=-1)
    result = jnp.zeros_like(column)
    for offset in range(4):
        first = ((shift_value + offset - 1) % lon_count).astype(jnp.int32)
        result = result + lon_w[offset] * lax.dynamic_slice_in_dim(doubled, first, lon_count, 2)
    return result


def reference(fields, lat_fraction, lon_fraction, lon_shift, departure_row, extents):
    row_ids = jnp.arange(NLAT, dtype=jnp.int32)
    band_ids = row_ids // ROWS
    low_bound = band_ids * ROWS - extents[band_ids, 0] * ROWS + 1
    high_bound = band_ids * ROWS + ROWS - 3 + extents[band_ids, 1] * ROWS
    departure = jnp.clip(jnp.clip(departure_row, low_bound, high_bound), 1, NLAT - 3).astype(jnp.int32)

    def one_row(inputs):
        dep_value, lat_t, lon_t, shift_value = inputs
        row_block = lax.dynamic_slice_in_dim(fields, (dep_value - 1).astype(jnp.int32), 4, 0)
        lat_w = cubic_weights(lat_t)
        column = lat_w[0] * row_block[0] + lat_w[1] * row_block[1] + lat_w[2] * row_block[2] + lat_w[3] * row_block[3]
        return along_lon(column, cubic_weights(lon_t), shift_value)

    moved = lax.map(one_row, (departure, lat_fraction, lon_fraction, lon_shift))
    area = jnp.cos(math.pi * (row_ids.astype(jnp.float32) + 0.5) / NLAT - math.pi / 2.0)
    mass_before = jnp.sum(area[:, None, None, None] * fields, axis=(0, 2, 3))
    mass_after = jnp.sum(area[:, None, None, None] * moved, axis=(0, 2, 3))
    return moved * (mass_before / mass_after)[None, :, None, None]
```

```python
import functools
import math

import jax
import jax.numpy as jnp
from jax import lax
from jax.experimental import pallas as pl
from jax.experimental.pallas import tpu as pltpu
from jax.sharding import PartitionSpec as P

REACH = 4
VMEM_LIMIT = 60 * 1024 * 1024


def send(block, flip=0, step=0):
    devices = range(lax.axis_size("lat"))
    route = [(i, (i ^ flip) + step) for i in devices if (i ^ flip) + step in devices]
    return lax.ppermute(block, "lat", route)


def cubic_weights(t):
    return (
        t * (t - 1.0) * (t - 2.0) * (-1.0 / 6.0),
        (t + 1.0) * (t - 1.0) * (t - 2.0) * 0.5,
        (t + 1.0) * t * (t - 2.0) * -0.5,
        (t + 1.0) * t * (t - 1.0) * (1.0 / 6.0),
    )


def add_bands(table, target, band_refs, band_ids, row_count, out_ref):
    lev_size = lax.axis_size("lev")
    last = lax.axis_size("lat") - 1
    line = jnp.clip(target, 0, last) * lev_size

    def row(r, carry):
        first = table[line, r].astype(jnp.int32) - 1
        weights = cubic_weights(table[line, row_count + r])
        for ref, band in zip(band_refs, band_ids):
            local = first - band * row_count

            @pl.when((local > -4) & (local < row_count))
            def _():
                total = out_ref[r]
                for a in range(4):
                    index = local + a
                    inside = (index >= 0) & (index < row_count)
                    weight = jnp.where(inside, weights[a], 0.0)
                    total = total + weight * ref[jnp.clip(index, 0, row_count - 1)]
                out_ref[r] = total

        return carry

    lax.fori_loop(0, row_count, row, 0)


def combine_kernel(offsets, targets, seeded, table, *refs):
    me = lax.axis_index("lat")
    bands = [(me ^ flip) + step for flip, step in offsets]
    band_refs = refs[: len(bands)]
    seeds = refs[len(bands) : len(bands) + sum(seeded)]
    outs = refs[len(bands) + sum(seeded) :]
    used = 0
    for (flip, step), seed, out in zip(targets, seeded, outs):
        if seed:
            out[...] = seeds[used][...]
            used += 1
        else:
            out[...] = jnp.zeros_like(out)
        add_bands(table, (me ^ flip) + step, band_refs, bands, out.shape[0], out)


def combine(table, bands, offsets, targets, seeds=None):
    seeds = seeds or [None] * len(targets)
    seeded = tuple(s is not None for s in seeds)
    operands = list(bands) + [s for s in seeds if s is not None]
    shape = bands[0].shape
    size = math.prod(shape)
    return pl.pallas_call(
        functools.partial(combine_kernel, tuple(offsets), tuple(targets), seeded),
        out_shape=[jax.ShapeDtypeStruct(shape, jnp.float32)] * len(targets),
        in_specs=[pl.BlockSpec(memory_space=pltpu.SMEM)]
        + [pl.BlockSpec(memory_space=pltpu.VMEM)] * len(operands),
        out_specs=[pl.BlockSpec(memory_space=pltpu.VMEM)] * len(targets),
        compiler_params=pltpu.CompilerParams(vmem_limit_bytes=VMEM_LIMIT),
        cost_estimate=pl.CostEstimate(
            flops=8 * size * len(targets),
            bytes_accessed=4 * size * (len(operands) + len(targets)),
            transcendentals=0,
        ),
    )(table, *operands)


def finish_kernel(split, table, shifts, ratio, *refs):
    pieces, out = refs[:-1], refs[-1]
    me = lax.axis_index("lat") * lax.axis_size("lev")
    row_count = pl.num_programs(0)
    r = pl.program_id(0)
    weights = cubic_weights(table[me, 2 * row_count + r])
    lon_count = out.shape[-1]
    base = shifts[r] - 1
    turn = jnp.where(base < 0, -base, lon_count - base)
    turn = jnp.where(turn == lon_count, 0, turn)
    start = 0
    for field, count in enumerate(split):
        column = pieces[start][0]
        for piece in pieces[start + 1 : start + count]:
            column = column + piece[0]
        start += count
        scaled = [w * ratio[field] for w in weights]
        moved = scaled[0] * column
        for k in range(1, 4):
            moved = moved + scaled[k] * pltpu.roll(column, lon_count - k, axis=1)
        out[0, field] = pltpu.roll(moved, turn, axis=1)


def finish(table, shifts, ratio, pieces):
    split = tuple(len(p) for p in pieces)
    flat = [x for p in pieces for x in p]
    row_count, lev_count, lon_count = flat[0].shape
    size = math.prod(flat[0].shape)
    smem = pl.BlockSpec(memory_space=pltpu.SMEM)
    return pl.pallas_call(
        functools.partial(finish_kernel, split),
        grid=(row_count,),
        out_shape=jax.ShapeDtypeStruct((row_count, len(pieces), lev_count, lon_count), jnp.float32),
        in_specs=[smem] * 3
        + [pl.BlockSpec((1, lev_count, lon_count), lambda r: (r, 0, 0))] * len(flat),
        out_specs=pl.BlockSpec((1, len(pieces), lev_count, lon_count), lambda r: (r, 0, 0, 0)),
        compiler_params=pltpu.CompilerParams(vmem_limit_bytes=VMEM_LIMIT),
        cost_estimate=pl.CostEstimate(
            flops=20 * size * len(pieces),
            bytes_accessed=4 * size * (len(flat) + len(pieces)),
            transcendentals=0,
        ),
    )(table, shifts, ratio, *flat)


def mass_ratio(table, row_count, field_count):
    band_count, lev_size = lax.axis_size("lat"), lax.axis_size("lev")
    total_rows = band_count * row_count
    parts = table.reshape(band_count, lev_size, -1)
    columns = [parts[:, 0, k * row_count : (k + 1) * row_count].reshape(total_rows) for k in range(3)]
    first = columns[0].astype(jnp.int32) - 1
    lat_w = cubic_weights(columns[1])
    lon_w = cubic_weights(columns[2])
    sums = parts[:, :, 3 * row_count :].sum(1).reshape(total_rows, field_count)
    row_ids = jnp.arange(total_rows, dtype=jnp.int32)
    area = jnp.cos(math.pi * (row_ids.astype(jnp.float32) + 0.5) / total_rows - math.pi / 2.0)
    gain = area * (lon_w[0] + lon_w[1] + lon_w[2] + lon_w[3])
    hit = jnp.zeros((total_rows, total_rows), jnp.float32)
    for a in range(4):
        hit = hit + jnp.where((first + a)[:, None] == row_ids[None, :], (gain * lat_w[a])[:, None], 0.0)
    after_w = hit.sum(0)
    before = (area[:, None] * sums).sum(0)
    after = (after_w[:, None] * sums).sum(0)
    return before / after


def per_device(fields, lat_fraction, lon_fraction, lon_shift, departure_row, extents):
    row_count, field_count = fields.shape[:2]
    band_count, lev_size = lax.axis_size("lat"), lax.axis_size("lev")
    first_row = lax.axis_index("lat") * row_count
    low_bound = first_row - extents[0, 0] * row_count + 1
    high_bound = first_row + row_count - 3 + extents[0, 1] * row_count
    departure = jnp.clip(jnp.clip(departure_row, low_bound, high_bound), 1, band_count * row_count - 3)

    near, middle, far = 1, 2, REACH
    both = near | middle
    f0, f1, f2 = (fields[:, f] for f in range(field_count))
    f0_north = send(f0, step=far)
    f1_near = send(f1, flip=near)
    f2_middle = send(f2, flip=middle)
    f0_south = send(f0, step=-far)
    sums = fields.sum((2, 3)).reshape(-1)
    mine = jnp.concatenate([departure.astype(jnp.float32), lat_fraction, lon_fraction, sums])
    copies = jnp.broadcast_to(mine[None], (band_count * lev_size, mine.shape[0]))
    table = lax.all_to_all(copies, ("lat", "lev"), 0, 0, tiled=True)

    f1_middle = send(f1, flip=middle)
    f2_north = send(f2, step=far)
    f2_south = send(f2, step=-far)
    f1_both = send(f1_near, flip=middle)
    f2_north_middle = send(f2_middle, step=far)
    f2_south_middle = send(f2_middle, step=-far)

    f0_bands = [f0_north, f0, f0_south]
    f0_at = [(0, -far), (0, 0), (0, far)]
    for_both, for_near = combine(table, f0_bands, f0_at, [(both, 0), (near, 0)])
    f0_relay = send(for_both, flip=near)
    f0_from_near = send(for_near, flip=near)
    (f0_own,) = combine(table, f0_bands, f0_at, [(0, 0)])
    (for_middle,) = combine(table, f0_bands, f0_at, [(middle, 0)], [f0_relay])
    f0_from_middle = send(for_middle, flip=middle)

    f1_bands = [f1, f1_near, f1_middle, f1_both]
    f1_at = [(0, 0), (near, 0), (middle, 0), (both, 0)]
    for_south, for_north = combine(table, f1_bands, f1_at, [(0, far), (0, -far)])
    f1_from_north = send(for_south, step=far)
    f1_from_south = send(for_north, step=-far)
    (f1_own,) = combine(table, f1_bands, f1_at, [(0, 0)])

    f2_bands = [f2, f2_middle, f2_north, f2_south, f2_north_middle, f2_south_middle]
    f2_at = [(0, 0), (middle, 0), (0, -far), (0, far), (middle, -far), (middle, far)]
    (f2_for_near,) = combine(table, f2_bands, f2_at, [(near, 0)])
    f2_from_near = send(f2_for_near, flip=near)
    (f2_own,) = combine(table, f2_bands, f2_at, [(0, 0)])

    ratio = mass_ratio(table, row_count, field_count)
    pieces = [
        [f0_own, f0_from_near, f0_from_middle],
        [f1_own, f1_from_north, f1_from_south],
        [f2_own, f2_from_near],
    ]
    return finish(table, lon_shift, ratio, pieces)


def solution(mesh):
    return jax.shard_map(
        per_device,
        mesh=mesh,
        in_specs=(
            P("lat", None, "lev", None),
            P("lat"),
            P("lat"),
            P("lat"),
            P("lat"),
            P("lat", None),
        ),
        out_specs=P("lat", None, "lev", None),
        check_vma=False,
    )
```

```python
import functools
import math

import jax
import jax.numpy as jnp
from jax import lax
from jax.experimental import pallas as pl
from jax.experimental.pallas import tpu as pltpu
from jax.sharding import PartitionSpec as P

REACH = 4
LANES = 128
VMEM_LIMIT = 12 * 1024 * 1024


def send(block, flip=0, step=0):
    devices = range(lax.axis_size("lat"))
    route = [(i, (i ^ flip) + step) for i in devices if (i ^ flip) + step in devices]
    return lax.ppermute(block, "lat", route)


def cubic_weights(t):
    return (
        t * (t - 1.0) * (t - 2.0) * (-1.0 / 6.0),
        (t + 1.0) * (t - 1.0) * (t - 2.0) * 0.5,
        (t + 1.0) * t * (t - 2.0) * -0.5,
        (t + 1.0) * t * (t - 1.0) * (1.0 / 6.0),
    )


def vmem():
    return pl.BlockSpec(memory_space=pltpu.VMEM)


def smem():
    return pl.BlockSpec(memory_space=pltpu.SMEM)


def cost(operands, results, flops):
    size = math.prod(results[0].shape)
    count = len(operands) + len(results)
    return pl.CostEstimate(flops=flops * size, bytes_accessed=4 * size * count, transcendentals=0)


def start_kernel(departure_row, lat_fraction, lon_fraction, extents, fields, *outs):
    parts, mine = outs[:-1], outs[-1]
    row_count = fields.shape[0]
    lanes = fields.shape[-1]
    first_row = lax.axis_index("lat") * row_count
    low_bound = first_row - extents[0, 0] * row_count + 1
    high_bound = first_row + row_count - 3 + extents[0, 1] * row_count
    last = lax.axis_size("lat") * row_count - 3
    at = lax.broadcasted_iota(jnp.int32, (1, mine.shape[-1]), 1)
    line = jnp.zeros((1, mine.shape[-1]), jnp.float32)
    for r in range(row_count):
        departure = jnp.clip(jnp.clip(departure_row[r], low_bound, high_bound), 1, last)
        line = jnp.where(at == r, departure.astype(jnp.float32), line)
        line = jnp.where(at == row_count + r, lat_fraction[r], line)
        line = jnp.where(at == 2 * row_count + r, lon_fraction[r], line)
    for r in range(row_count):
        for f, part in enumerate(parts):
            row = fields[r, f]
            part[r] = row
            tiles = [row[:, k : k + LANES] for k in range(0, lanes, LANES)]
            while len(tiles) > 1:
                tiles = [sum(tiles[k : k + 2]) for k in range(0, len(tiles), 2)]
            line = jnp.where(at == 3 * row_count + r * len(parts) + f, jnp.sum(tiles[0]), line)
    mine[...] = jnp.broadcast_to(line[None], mine.shape)


def start(departure_row, lat_fraction, lon_fraction, extents, fields):
    row_count, field_count, lev_count, lon_count = fields.shape
    part = jax.ShapeDtypeStruct((row_count, lev_count, lon_count), jnp.float32)
    width = pl.cdiv((3 + field_count) * row_count, LANES) * LANES
    copies = lax.axis_size("lat") * lax.axis_size("lev")
    outs = [part] * field_count + [jax.ShapeDtypeStruct((copies, 1, width), jnp.float32)]
    return pl.pallas_call(
        start_kernel,
        out_shape=outs,
        in_specs=[smem()] * 4 + [vmem()],
        out_specs=[vmem()] * len(outs),
        compiler_params=pltpu.CompilerParams(vmem_limit_bytes=VMEM_LIMIT),
        cost_estimate=cost([part] * field_count, [part] * field_count, 3),
    )(departure_row, lat_fraction, lon_fraction, extents, fields)


def add_bands(table, target, band_refs, band_ids, row_count, out_ref):
    line = jnp.clip(target, 0, lax.axis_size("lat") - 1) * lax.axis_size("lev")

    def row(r, carry):
        first = table[line, r].astype(jnp.int32) - 1
        weights = cubic_weights(table[line, row_count + r])
        for ref, band in zip(band_refs, band_ids):
            local = first - band * row_count

            @pl.when((local > -4) & (local < row_count))
            def _():
                total = out_ref[r]
                for a in range(4):
                    index = local + a
                    inside = (index >= 0) & (index < row_count)
                    weight = jnp.where(inside, weights[a], 0.0)
                    total = total + weight * ref[jnp.clip(index, 0, row_count - 1)]
                out_ref[r] = total

        return carry

    lax.fori_loop(0, row_count, row, 0)


def combine_kernel(offsets, targets, seeded, table, *refs):
    me = lax.axis_index("lat")
    bands = [place(me) for place in offsets]
    band_refs = refs[: len(bands)]
    seeds = refs[len(bands) : len(bands) + sum(seeded)]
    outs = refs[len(bands) + sum(seeded) :]
    used = 0
    for place, seed, out in zip(targets, seeded, outs):
        if seed:
            out[...] = seeds[used][...]
            used += 1
        else:
            out[...] = jnp.zeros_like(out)
        add_bands(table, place(me), band_refs, bands, out.shape[0], out)


def at(flip=0, step=0):
    return lambda me: (me ^ flip) + step


def combine(table, bands, offsets, targets, seeds=None):
    seeds = seeds or [None] * len(targets)
    seeded = tuple(s is not None for s in seeds)
    operands = list(bands) + [s for s in seeds if s is not None]
    outs = [jax.ShapeDtypeStruct(bands[0].shape, jnp.float32)] * len(targets)
    return pl.pallas_call(
        functools.partial(combine_kernel, offsets, targets, seeded),
        out_shape=outs,
        in_specs=[smem()] + [vmem()] * len(operands),
        out_specs=[vmem()] * len(outs),
        compiler_params=pltpu.CompilerParams(vmem_limit_bytes=VMEM_LIMIT),
        cost_estimate=cost(operands, outs, 8 * len(outs)),
    )(table, *operands)


def finish_kernel(split, table, shifts, ratio, *refs):
    pieces, out, twice, ready, sems = refs[:-4], refs[-4], refs[-3], refs[-2], refs[-1]
    me = lax.axis_index("lat") * lax.axis_size("lev")
    row_count = ready.shape[0]
    lon_count = out.shape[-1]
    tile_count = lon_count // LANES
    lane = lax.broadcasted_iota(jnp.int32, (out.shape[-2], LANES), 1)

    def ship(r):
        return pltpu.make_async_copy(ready.at[r], out.at[r], sems.at[r])

    def row(r, carry):
        weights = cubic_weights(table[me, 2 * row_count + r])
        base = shifts[r] - 1
        base = jnp.where(base < 0, base + lon_count, base)
        start = 0
        for field, count in enumerate(split):
            column = pieces[start][r]
            for piece in pieces[start + 1 : start + count]:
                column = column + piece[r]
            start += count
            twice[field, :, :lon_count] = column
            twice[field, :, lon_count : 2 * lon_count] = column
            twice[field, :, 2 * lon_count :] = column[:, :LANES]
        for field in range(len(split)):
            moved = [None] * tile_count
            for k in range(4):
                first = (base + k) // LANES
                turn = (base + k) % LANES
                weight = weights[k] * ratio[field]
                keep = lane < LANES - turn
                back = jnp.where(turn == 0, 0, LANES - turn)
                tiles = [
                    pltpu.roll(
                        twice[field, :, pl.ds(pl.multiple_of((first + n) * LANES, LANES), LANES)],
                        back,
                        axis=1,
                    )
                    for n in range(tile_count + 1)
                ]
                for n in range(tile_count):
                    term = weight * jnp.where(keep, tiles[n], tiles[n + 1])
                    moved[n] = term if k == 0 else moved[n] + term
            for n in range(tile_count):
                ready[r, field, :, n * LANES : (n + 1) * LANES] = moved[n]

        @pl.when(r > 0)
        def _():
            ship(r - 1).start()

        return carry

    lax.fori_loop(0, row_count, row, 0)
    ship(row_count - 1).start()
    for r in range(row_count):
        ship(r).wait()


def finish(table, shifts, ratio, pieces):
    split = tuple(len(p) for p in pieces)
    flat = [x for p in pieces for x in p]
    row_count, lev_count, lon_count = flat[0].shape
    out = jax.ShapeDtypeStruct((row_count, len(pieces), lev_count, lon_count), jnp.float32)
    return pl.pallas_call(
        functools.partial(finish_kernel, split),
        out_shape=out,
        in_specs=[smem()] * 3 + [vmem()] * len(flat),
        out_specs=pl.BlockSpec(memory_space=pl.ANY),
        scratch_shapes=[
            pltpu.VMEM((len(pieces), lev_count, 2 * lon_count + LANES), jnp.float32),
            pltpu.VMEM(out.shape, jnp.float32),
            pltpu.SemaphoreType.DMA((row_count,)),
        ],
        compiler_params=pltpu.CompilerParams(vmem_limit_bytes=VMEM_LIMIT),
        cost_estimate=cost(flat, [out], 20),
    )(table, shifts, ratio, *flat)


def mass_ratio(table, row_count, field_count):
    band_count, lev_size = lax.axis_size("lat"), lax.axis_size("lev")
    total_rows = band_count * row_count
    parts = table.reshape(band_count, lev_size, -1)
    columns = [parts[:, 0, k * row_count : (k + 1) * row_count].reshape(total_rows) for k in range(3)]
    first = columns[0].astype(jnp.int32) - 1
    lat_w = cubic_weights(columns[1])
    lon_w = cubic_weights(columns[2])
    sums = parts[:, :, 3 * row_count : (3 + field_count) * row_count].sum(1).reshape(total_rows, field_count)
    row_ids = jnp.arange(total_rows, dtype=jnp.int32)
    area = jnp.cos(math.pi * (row_ids.astype(jnp.float32) + 0.5) / total_rows - math.pi / 2.0)
    gain = area * (lon_w[0] + lon_w[1] + lon_w[2] + lon_w[3])
    hit = jnp.zeros((total_rows, total_rows), jnp.float32)
    for a in range(4):
        hit = hit + jnp.where((first + a)[:, None] == row_ids[None, :], (gain * lat_w[a])[:, None], 0.0)
    after_w = hit.sum(0)
    before = (area[:, None] * sums).sum(0)
    after = (after_w[:, None] * sums).sum(0)
    return before / after


def per_device(fields, lat_fraction, lon_fraction, lon_shift, departure_row, extents):
    row_count, field_count = fields.shape[:2]
    near, middle, far = 1, 2, REACH
    both = near | middle
    devices = range(lax.axis_size("lat"))
    f0, f1, f2, mine = start(departure_row, lat_fraction, lon_fraction, extents, fields)
    table = lax.all_to_all(mine, ("lat", "lev"), 0, 0, tiled=True).reshape(mine.shape[0], -1)
    f0_north = send(f0, step=far)
    f0_south = send(f0, step=-far)
    f1_near = send(f1, flip=near)
    f2_middle = send(f2, flip=middle)
    f1_middle = send(f1, flip=middle)
    f2_north = send(f2, step=far)
    f2_south = send(f2, step=-far)

    f0_bands = [f0_north, f0, f0_south]
    f0_at = [at(step=-far), at(), at(step=far)]
    (for_both,) = combine(table, f0_bands, f0_at, [at(both)])
    f0_relay = send(for_both, flip=near)
    (for_near,) = combine(table, f0_bands, f0_at, [at(near)])
    f0_from_near = send(for_near, flip=near)

    f1_both = send(f1_near, flip=middle)
    side = [(i, i - far if i & middle else i + far) for i in devices]
    f2_side = lax.ppermute(f2_middle, "lat", [(i, j) for i, j in side if j in devices])

    def side_at(me):
        return jnp.where((me & middle) != 0, (me ^ middle) + far, (me ^ middle) - far)

    (f0_own,) = combine(table, f0_bands, f0_at, [at()])
    (for_middle,) = combine(table, f0_bands, f0_at, [at(middle)], [f0_relay])
    f0_from_middle = send(for_middle, flip=middle)

    f1_bands = [f1, f1_near, f1_middle]
    f1_at = [at(), at(near), at(middle)]
    early = combine(table, f1_bands, f1_at, [at(step=far), at(step=-far), at()])
    for_south, for_north = combine(table, [f1_both], [at(both)], [at(step=far), at(step=-far)], early[:2])
    f1_from_north = send(for_south, step=far)
    f1_from_south = send(for_north, step=-far)
    (f1_own,) = combine(table, [f1_both], [at(both)], [at()], early[2:])

    f2_bands = [f2, f2_middle, f2_north, f2_south]
    f2_at = [at(), at(middle), at(step=-far), at(step=far)]
    early = combine(table, f2_bands, f2_at, [at(near), at()])
    (f2_for_near,) = combine(table, [f2_side], [side_at], [at(near)], early[:1])
    f2_from_near = send(f2_for_near, flip=near)
    (f2_own,) = combine(table, [f2_side], [side_at], [at()], early[1:])

    ratio = mass_ratio(table, row_count, field_count)
    pieces = [
        [f0_own, f0_from_near, f0_from_middle],
        [f1_own, f1_from_north, f1_from_south],
        [f2_own, f2_from_near],
    ]
    return finish(table, lon_shift, ratio, pieces)


def solution(mesh):
    return jax.shard_map(
        per_device,
        mesh=mesh,
        in_specs=(
            P("lat", None, "lev", None),
            P("lat"),
            P("lat"),
            P("lat"),
            P("lat"),
            P("lat", None),
        ),
        out_specs=P("lat", None, "lev", None),
        check_vma=False,
    )
```

```python
import functools
import math

import jax
import jax.numpy as jnp
from jax import lax
from jax.experimental import pallas as pl
from jax.experimental.pallas import tpu as pltpu
from jax.sharding import PartitionSpec as P


REACH = 4
LANES = 128
VMEM_LIMIT = 12 * 1024 * 1024
START_LIMIT = 60 * 1024 * 1024


def flip(mask):
    return lambda me: me ^ mask


def stay(me):
    return me


def across(me):
    return ((me + REACH) ^ REACH) - REACH


def onward(me):
    return me + REACH * (1 - (me & 2))


def back(me):
    return me - REACH * (1 - (me & 2))


def side(me):
    return back(me) ^ 2


def send(block, place):
    devices = range(lax.axis_size("lat"))
    route = [(i, place(i)) for i in devices if place(i) in devices]
    return lax.ppermute(block, "lat", route)


def cubic_weights(t):
    return (
        t * (t - 1.0) * (t - 2.0) * (-1.0 / 6.0),
        (t + 1.0) * (t - 1.0) * (t - 2.0) * 0.5,
        (t + 1.0) * t * (t - 2.0) * -0.5,
        (t + 1.0) * t * (t - 1.0) * (1.0 / 6.0),
    )


def vmem():
    return pl.BlockSpec(memory_space=pltpu.VMEM)


def smem():
    return pl.BlockSpec(memory_space=pltpu.SMEM)


def hbm():
    return pl.BlockSpec(memory_space=pltpu.HBM)


def from_hbm(array):
    return pltpu.with_memory_space_constraint(array, pltpu.HBM)


def cost(operands, results, flops):
    size = math.prod(results[0].shape)
    count = len(operands) + len(results)
    return pl.CostEstimate(flops=flops * size, bytes_accessed=4 * size * count, transcendentals=0)


def start_kernel(departure_row, lat_fraction, lon_fraction, extents, fields, *refs):
    parts, plan = refs[:-11], refs[-11]
    departure_s, lat_s, lon_s, extents_s, held, ready, tile_s = refs[-10:-3]
    sems, in_sems, out_sems = refs[-3:]
    row_count, field_count, lev_count, lon_count = fields.shape
    tile_count = lon_count // LANES
    scalars = (departure_row, lat_fraction, lon_fraction, extents)
    copies = [
        pltpu.make_async_copy(source, target, sems.at[k])
        for k, (source, target) in enumerate(zip(scalars, (departure_s, lat_s, lon_s, extents_s)))
    ]
    rows = [pltpu.make_async_copy(fields.at[r], held.at[r], in_sems.at[r]) for r in range(row_count)]
    for copy in copies + rows:
        copy.start()
    for copy in copies:
        copy.wait()
    first_row = lax.axis_index("lat") * row_count
    low_bound = first_row - extents_s[0, 0] * row_count + 1
    high_bound = first_row + row_count - 3 + extents_s[0, 1] * row_count
    last = lax.axis_size("lat") * row_count - 3
    at = lax.broadcasted_iota(jnp.int32, (lev_count, LANES), 1)
    tile = jnp.zeros((lev_count, LANES), jnp.float32)
    for r in range(row_count):
        departure = jnp.clip(jnp.clip(departure_s[r], low_bound, high_bound), 1, last)
        tile = jnp.where(at == r, departure.astype(jnp.float32), tile)
        tile = jnp.where(at == row_count + r, lat_s[r], tile)
        tile = jnp.where(at == 2 * row_count + r, lon_s[r], tile)
    tile_s[...] = tile
    plan[0] = tile
    ships = []
    for f, part in enumerate(parts):
        ships.append(pltpu.make_async_copy(tile_s, part.at[row_count * tile_count], out_sems.at[f, row_count]))
    for r in range(row_count):
        rows[r].wait()
        for ship in ships[-field_count:]:
            ship.start()
        for f, part in enumerate(parts):
            for n in range(tile_count):
                ready[f, r * tile_count + n] = held[r, f, :, n * LANES : (n + 1) * LANES]
            span = pl.ds(r * tile_count, tile_count)
            ships.append(pltpu.make_async_copy(ready.at[f, span], part.at[span], out_sems.at[f, r]))
    for ship in ships[-field_count:]:
        ship.start()
    for ship in ships:
        ship.wait()


def start(departure_row, lat_fraction, lon_fraction, extents, fields):
    row_count, field_count, lev_count, lon_count = fields.shape
    tiles = row_count * lon_count // LANES
    part = jax.ShapeDtypeStruct((tiles + 1, lev_count, LANES), jnp.float32)
    plan = jax.ShapeDtypeStruct((1, lev_count, LANES), jnp.float32)
    return pl.pallas_call(
        start_kernel,
        out_shape=[part] * field_count + [plan],
        in_specs=[hbm()] * 5,
        out_specs=[hbm()] * field_count + [vmem()],
        scratch_shapes=[
            pltpu.SMEM(departure_row.shape, jnp.int32),
            pltpu.SMEM(lat_fraction.shape, jnp.float32),
            pltpu.SMEM(lon_fraction.shape, jnp.float32),
            pltpu.SMEM(extents.shape, jnp.int32),
            pltpu.VMEM(fields.shape, jnp.float32),
            pltpu.VMEM((field_count, tiles, lev_count, LANES), jnp.float32),
            pltpu.VMEM((lev_count, LANES), jnp.float32),
            pltpu.SemaphoreType.DMA((4,)),
            pltpu.SemaphoreType.DMA((row_count,)),
            pltpu.SemaphoreType.DMA((field_count, row_count + 1)),
        ],
        compiler_params=pltpu.CompilerParams(vmem_limit_bytes=START_LIMIT),
        cost_estimate=cost([part] * field_count, [part] * field_count, 3),
    )(departure_row, lat_fraction, lon_fraction, extents, fields)


def sums_kernel(row_count, *refs):
    parts, mine = refs[:-1], refs[-1]
    tile_count = parts[0].shape[0] // row_count
    at = lax.broadcasted_iota(jnp.int32, (1, LANES), 1)
    line = parts[0][row_count * tile_count][:1]
    for r in range(row_count):
        for f, part in enumerate(parts):
            tiles = [part[r * tile_count + n] for n in range(tile_count)]
            while len(tiles) > 1:
                tiles = [sum(tiles[k : k + 2]) for k in range(0, len(tiles), 2)]
            line = jnp.where(at == 3 * row_count + r * len(parts) + f, jnp.sum(tiles[0]), line)
    mine[...] = jnp.broadcast_to(line[None], mine.shape)


def exchange(parts, row_count):
    copies = lax.axis_size("lat") * lax.axis_size("lev")
    mine = pl.pallas_call(
        functools.partial(sums_kernel, row_count),
        out_shape=jax.ShapeDtypeStruct((copies, 1, LANES), jnp.float32),
        in_specs=[vmem()] * len(parts),
        out_specs=vmem(),
        compiler_params=pltpu.CompilerParams(vmem_limit_bytes=VMEM_LIMIT),
        cost_estimate=cost(parts, parts[:1], 3),
    )(*parts)
    return lax.all_to_all(mine, ("lat", "lev"), 0, 0, tiled=True)


def collect_kernel(*refs):
    parts, tiles, sems = refs[:-2], refs[-2], refs[-1]
    copies = [
        pltpu.make_async_copy(part.at[part.shape[0] - 1], tiles.at[k], sems.at[k])
        for k, part in enumerate(parts)
    ]
    for copy in copies:
        copy.start()
    for copy in copies:
        copy.wait()


def collect(parts):
    return pl.pallas_call(
        collect_kernel,
        out_shape=jax.ShapeDtypeStruct((len(parts),) + parts[0].shape[1:], jnp.float32),
        in_specs=[hbm()] * len(parts),
        out_specs=vmem(),
        scratch_shapes=[pltpu.SemaphoreType.DMA((len(parts),))],
        compiler_params=pltpu.CompilerParams(vmem_limit_bytes=VMEM_LIMIT),
        cost_estimate=pl.CostEstimate(flops=1000, bytes_accessed=8000, transcendentals=0),
    )(*parts)


def add_bands(plan, band_refs, band_ids, row_count, out_ref):
    tile_count = out_ref.shape[0] // row_count

    def row(r, carry):
        first = plan[0, r].astype(jnp.int32) - 1
        weights = cubic_weights(plan[0, row_count + r])
        for ref, band in zip(band_refs, band_ids):
            local = first - band * row_count

            @pl.when((local > -4) & (local < row_count))
            def _():
                total = out_ref[pl.ds(r * tile_count, tile_count)]
                for a in range(4):
                    index = local + a
                    inside = (index >= 0) & (index < row_count)
                    weight = jnp.where(inside, weights[a], 0.0)
                    index = jnp.clip(index, 0, row_count - 1)
                    total = total + weight * ref[pl.ds(index * tile_count, tile_count)]
                out_ref[pl.ds(r * tile_count, tile_count)] = total

        return carry

    lax.fori_loop(0, row_count, row, 0)


def combine_kernel(row_count, jobs, *refs):
    me = lax.axis_index("lat")
    outs = refs[len(refs) - len(jobs) :]
    for (bands, places, plan, line, seed), out in zip(jobs, outs):
        out[...] = jnp.zeros_like(out) if seed is None else refs[seed][pl.ds(0, out.shape[0])]
        band_ids = [place(me) for place in places]
        add_bands(refs[plan].at[line(me)], [refs[b] for b in bands], band_ids, row_count, out)


def combine(row_count, *jobs):
    scalars, arrays = [], []

    def index(array, known):
        for k, other in enumerate(known):
            if other is array:
                return k
        known.append(array)
        return len(known) - 1

    kept = []
    for bands, places, (plan, line), *seed in jobs:
        held = [index(b, arrays) for b in bands]
        kept.append((held, places, index(plan, scalars), line, index(seed[0], arrays) if seed else None))
    shift = len(scalars)
    kept = [
        ([b + shift for b in held], places, plan, line, None if seed is None else seed + shift)
        for held, places, plan, line, seed in kept
    ]
    tiles, lev_count, _ = jobs[0][0][0].shape
    outs = [jax.ShapeDtypeStruct((tiles - 1, lev_count, LANES), jnp.float32)] * len(jobs)
    return pl.pallas_call(
        functools.partial(combine_kernel, row_count, kept),
        out_shape=outs,
        in_specs=[smem()] * len(scalars) + [vmem()] * len(arrays),
        out_specs=[vmem()] * len(outs),
        compiler_params=pltpu.CompilerParams(vmem_limit_bytes=VMEM_LIMIT),
        cost_estimate=cost(arrays, outs, 8 * len(outs)),
    )(*scalars, *arrays)


def finish_kernel(split, plan, shifts, ratio, *refs):
    pieces = refs[: sum(len(held) for _, held in split)]
    out, kept, twice, ready, plan_s, shifts_s, ratio_s, scalar_sems, in_sems, sems = refs[-10:]
    row_count, lev_count, lon_count = ready.shape[1:]
    tile_count = lon_count // LANES
    group = twice.shape[0]
    lane = lax.broadcasted_iota(jnp.int32, (lev_count, LANES), 1)
    scalars = [
        pltpu.make_async_copy(source, target, scalar_sems.at[k])
        for k, (source, target) in enumerate(zip((plan, shifts, ratio), (plan_s, shifts_s, ratio_s)))
    ]

    def fetch(p, step):
        span = pl.ds(step * group * tile_count, group * tile_count)
        return pltpu.make_async_copy(pieces[p].at[span], kept.at[p, span], in_sems.at[p, step])

    for copy in scalars:
        copy.start()
    for _, held in split:
        for step in range(row_count // group):
            for p in held:
                fetch(p, step).start()
    for copy in scalars:
        copy.wait()

    for k, (field, held) in enumerate(split):

        def ship(r):
            return pltpu.make_async_copy(ready.at[k, r], out.at[r, field], sems.at[k, r])

        def rows(step, carry):
            for p in held:
                fetch(p, step).wait()
            for u in range(group):
                span = pl.ds((step * group + u) * tile_count, tile_count)
                column = kept[held[0], span]
                for p in held[1:]:
                    column = column + kept[p, span]
                twice[u, :tile_count] = column
                twice[u, tile_count : 2 * tile_count] = column
                twice[u, 2 * tile_count] = column[0]
            for u in range(group):
                r = step * group + u
                weights = cubic_weights(plan_s[0, 0, 2 * row_count + r])
                base = shifts_s[r] - 1
                base = jnp.where(base < 0, base + lon_count, base)
                moved = [None] * tile_count
                for tap in range(4):
                    first = (base + tap) // LANES
                    turn = (base + tap) % LANES
                    weight = weights[tap] * ratio_s[field]
                    keep = lane < LANES - turn
                    shift = jnp.where(turn == 0, 0, LANES - turn)
                    tiles = [pltpu.roll(twice[u, first + n], shift, axis=1) for n in range(tile_count + 1)]
                    for n in range(tile_count):
                        term = weight * jnp.where(keep, tiles[n], tiles[n + 1])
                        moved[n] = term if tap == 0 else moved[n] + term
                for n in range(tile_count):
                    ready[k, r, :, n * LANES : (n + 1) * LANES] = moved[n]

            @pl.when(step > 0)
            def _():
                for u in range(group):
                    ship((step - 1) * group + u).start()

            return carry

        lax.fori_loop(0, row_count // group, rows, 0)
        for u in range(group):
            ship(row_count - group + u).start()
    for k, (field, _) in enumerate(split):
        for r in range(row_count):
            pltpu.make_async_copy(ready.at[k, r], out.at[r, field], sems.at[k, r]).wait()


def finish(plan, shifts, ratio, pieces, out_shape, out=None):
    row_count, _, lev_count, lon_count = out_shape
    given = [] if out is None else [out]
    group = next(g for g in (5, 4, 3, 2, 1) if row_count % g == 0)
    flat, split = [], []
    for field, parts in pieces.items():
        split.append((field, tuple(range(len(flat), len(flat) + len(parts)))))
        flat += parts
    return pl.pallas_call(
        functools.partial(finish_kernel, split),
        out_shape=jax.ShapeDtypeStruct(out_shape, jnp.float32),
        in_specs=[hbm()] * (3 + len(flat) + len(given)),
        out_specs=hbm(),
        input_output_aliases={3 + len(flat): 0} if given else {},
        scratch_shapes=[
            pltpu.VMEM((len(flat),) + flat[0].shape, jnp.float32),
            pltpu.VMEM((group, 2 * lon_count // LANES + 1, lev_count, LANES), jnp.float32),
            pltpu.VMEM((len(split), row_count, lev_count, lon_count), jnp.float32),
            pltpu.SMEM(plan.shape, plan.dtype),
            pltpu.SMEM(shifts.shape, shifts.dtype),
            pltpu.SMEM(ratio.shape, ratio.dtype),
            pltpu.SemaphoreType.DMA((3,)),
            pltpu.SemaphoreType.DMA((len(flat), row_count // group)),
            pltpu.SemaphoreType.DMA((len(split), row_count)),
        ],
        compiler_params=pltpu.CompilerParams(vmem_limit_bytes=VMEM_LIMIT),
        cost_estimate=cost(flat, flat[:1], 60 * len(split)),
    )(plan, shifts, ratio, *flat, *given)


def mass_ratio(table, row_count, field_count):
    band_count, lev_size = lax.axis_size("lat"), lax.axis_size("lev")
    total_rows = band_count * row_count
    parts = table.reshape(band_count, lev_size, -1)
    columns = [parts[:, 0, k * row_count : (k + 1) * row_count].reshape(total_rows) for k in range(3)]
    first = columns[0].astype(jnp.int32) - 1
    lat_w = cubic_weights(columns[1])
    lon_w = cubic_weights(columns[2])
    sums = parts[:, :, 3 * row_count : (3 + field_count) * row_count].sum(1).reshape(total_rows, field_count)
    row_ids = jnp.arange(total_rows, dtype=jnp.int32)
    area = jnp.cos(math.pi * (row_ids.astype(jnp.float32) + 0.5) / total_rows - math.pi / 2.0)
    gain = area * (lon_w[0] + lon_w[1] + lon_w[2] + lon_w[3])
    hit = jnp.zeros((total_rows, total_rows), jnp.float32)
    for a in range(4):
        hit = hit + jnp.where((first + a)[:, None] == row_ids[None, :], (gain * lat_w[a])[:, None], 0.0)
    after_w = hit.sum(0)
    before = (area[:, None] * sums).sum(0)
    after = (after_w[:, None] * sums).sum(0)
    return before / after


def one_step(fields, lat_fraction, lon_fraction, lon_shift, departure_row, extents):
    row_count, field_count = fields.shape[:2]
    near, middle, both = flip(1), flip(2), flip(3)
    even, odd = flip(REACH), across
    join = functools.partial(combine, row_count)
    f0, f1, f2, plan = start(departure_row, lat_fraction, lon_fraction, extents, fields)
    both_plan = send(plan, both)
    f2_middle = send(f2, middle)
    f0_even = send(f0, even)
    f0_odd = send(f0, odd)
    f1_near = send(f1, near)
    f1_middle = send(f1, middle)
    table = exchange([from_hbm(f) for f in (f0, f1, f2)], row_count)
    f2_even = send(f2, even)
    f2_odd = send(f2, odd)
    f1_both = send(f1_near, middle)
    f2_side = send(f2_middle, onward)

    f0, f1, f2 = (from_hbm(f) for f in (f0, f1, f2))
    plans = collect([f1_near, f2_middle, f0_even, f0_odd])
    near_plan, middle_plan = (plans, lambda me: 0), (plans, lambda me: 1)
    onward_plan = (plans, lambda me: jnp.where(onward(me) == even(me), 2, 3))
    back_plan = (plans, lambda me: jnp.where(back(me) == even(me), 2, 3))
    own_plan, far_plan = (plan, lambda me: 0), (both_plan, lambda me: 0)

    f0_all = [f0, f0_even, f0_odd], [stay, even, odd]
    (for_both,) = join((*f0_all, far_plan))
    f0_relay = send(for_both, near)
    (for_near,) = join((*f0_all, near_plan))
    f0_from_near = send(for_near, near)
    (for_middle,) = join((*f0_all, middle_plan, f0_relay))
    f0_from_middle = send(for_middle, middle)

    (for_back,) = join(([f1, f1_near], [stay, near], back_plan))
    f1_from_onward = send(for_back, back)
    f1_all = [f1, f1_near, f1_middle], [stay, near, middle]
    f1_early, f1_own = join((*f1_all, onward_plan), (*f1_all, own_plan))
    f2_all = [f2, f2_middle, f2_even, f2_odd], [stay, middle, even, odd]
    f2_early, f2_own = join((*f2_all, near_plan), (*f2_all, own_plan))
    (for_onward,) = join(([f1_both], [both], onward_plan, f1_early))
    f1_from_back = send(for_onward, onward)
    (f2_for_near,) = join(([f2_side], [side], near_plan, f2_early))
    f2_from_near = send(f2_for_near, near)
    (f0_own,) = join((*f0_all, own_plan, f0_from_near))
    (f1_own,) = join(([f1_both], [both], own_plan, f1_own))
    (f2_own,) = join(([f2_side], [side], own_plan, f2_own))

    ratio = mass_ratio(table, row_count, field_count)
    pieces = [f0_own, f0_from_middle], [f1_own, f1_from_onward, f1_from_back], [f2_own, f2_from_near]
    out = None
    for field, parts in enumerate(pieces):
        out = finish(plan, lon_shift, ratio, {field: parts}, fields.shape, out)
    return out


def solution(mesh):
    return jax.shard_map(
        one_step,
        mesh=mesh,
        in_specs=(
            P("lat", None, "lev", None),
            P("lat"),
            P("lat"),
            P("lat"),
            P("lat"),
            P("lat", None),
        ),
        out_specs=P("lat", None, "lev", None),
        check_vma=False,
    )
```

```python
import functools
import math

import jax
import jax.numpy as jnp
from jax import lax
from jax.experimental import pallas as pl
from jax.experimental.pallas import tpu as pltpu
from jax.sharding import PartitionSpec as P


REACH = 4
LANES = 128
VMEM_LIMIT = 28 * 1024 * 1024
START_LIMIT = 60 * 1024 * 1024


def flip(mask):
    return lambda me: me ^ mask


def stay(me):
    return me


def across(me):
    return ((me + REACH) ^ REACH) - REACH


def onward(me):
    return me + REACH * (1 - (me & 2))


def back(me):
    return me - REACH * (1 - (me & 2))


def side(me):
    return back(me) ^ 2


def send(block, place):
    devices = range(lax.axis_size("lat"))
    route = [(i, place(i)) for i in devices if place(i) in devices]
    return lax.ppermute(block, "lat", route)


def cubic_weights(t):
    return (
        t * (t - 1.0) * (t - 2.0) * (-1.0 / 6.0),
        (t + 1.0) * (t - 1.0) * (t - 2.0) * 0.5,
        (t + 1.0) * t * (t - 2.0) * -0.5,
        (t + 1.0) * t * (t - 1.0) * (1.0 / 6.0),
    )


def vmem():
    return pl.BlockSpec(memory_space=pltpu.VMEM)


def smem():
    return pl.BlockSpec(memory_space=pltpu.SMEM)


def hbm():
    return pl.BlockSpec(memory_space=pltpu.HBM)


def from_hbm(array):
    return pltpu.with_memory_space_constraint(array, pltpu.HBM)


def cost(operands, results, flops):
    size = math.prod(results[0].shape)
    count = len(operands) + len(results)
    return pl.CostEstimate(flops=flops * size, bytes_accessed=4 * size * count, transcendentals=0)


def start_kernel(chosen, departure_row, lat_fraction, lon_fraction, extents, fields, *refs):
    parts, plan = refs[:-11], refs[-11]
    departure_s, lat_s, lon_s, extents_s, held, ready, tile_s = refs[-10:-3]
    sems, in_sems, out_sems = refs[-3:]
    row_count, _, lev_count, lon_count = fields.shape
    field_count = len(chosen)
    tile_count = lon_count // LANES
    scalars = (departure_row, lat_fraction, lon_fraction, extents)
    copies = [
        pltpu.make_async_copy(source, target, sems.at[k])
        for k, (source, target) in enumerate(zip(scalars, (departure_s, lat_s, lon_s, extents_s)))
    ]
    rows = [
        [pltpu.make_async_copy(fields.at[r, f], held.at[k, r], in_sems.at[k, r]) for k, f in enumerate(chosen)]
        for r in range(row_count)
    ]
    for copy in sum(rows, copies):
        copy.start()
    for copy in copies:
        copy.wait()
    first_row = lax.axis_index("lat") * row_count
    low_bound = first_row - extents_s[0, 0] * row_count + 1
    high_bound = first_row + row_count - 3 + extents_s[0, 1] * row_count
    last = lax.axis_size("lat") * row_count - 3
    at = lax.broadcasted_iota(jnp.int32, (lev_count, LANES), 1)
    tile = jnp.zeros((lev_count, LANES), jnp.float32)
    for r in range(row_count):
        departure = jnp.clip(jnp.clip(departure_s[r], low_bound, high_bound), 1, last)
        tile = jnp.where(at == r, departure.astype(jnp.float32), tile)
        tile = jnp.where(at == row_count + r, lat_s[r], tile)
        tile = jnp.where(at == 2 * row_count + r, lon_s[r], tile)
    tile_s[...] = tile
    plan[0] = tile
    ships = []
    for f, part in enumerate(parts):
        ships.append(pltpu.make_async_copy(tile_s, part.at[row_count * tile_count], out_sems.at[f, row_count]))
    for r in range(row_count):
        for copy in rows[r]:
            copy.wait()
        for ship in ships[-field_count:]:
            ship.start()
        for f, part in enumerate(parts):
            for n in range(tile_count):
                ready[f, r * tile_count + n] = held[f, r, :, n * LANES : (n + 1) * LANES]
            span = pl.ds(r * tile_count, tile_count)
            ships.append(pltpu.make_async_copy(ready.at[f, span], part.at[span], out_sems.at[f, r]))
    for ship in ships[-field_count:]:
        ship.start()
    for ship in ships:
        ship.wait()


def start(chosen, departure_row, lat_fraction, lon_fraction, extents, fields):
    row_count, _, lev_count, lon_count = fields.shape
    field_count = len(chosen)
    tiles = row_count * lon_count // LANES
    part = jax.ShapeDtypeStruct((tiles + 1, lev_count, LANES), jnp.float32)
    plan = jax.ShapeDtypeStruct((1, lev_count, LANES), jnp.float32)
    return pl.pallas_call(
        functools.partial(start_kernel, chosen),
        out_shape=[part] * field_count + [plan],
        in_specs=[hbm()] * 5,
        out_specs=[hbm()] * field_count + [vmem()],
        scratch_shapes=[
            pltpu.SMEM(departure_row.shape, jnp.int32),
            pltpu.SMEM(lat_fraction.shape, jnp.float32),
            pltpu.SMEM(lon_fraction.shape, jnp.float32),
            pltpu.SMEM(extents.shape, jnp.int32),
            pltpu.VMEM((field_count, row_count, lev_count, lon_count), jnp.float32),
            pltpu.VMEM((field_count, tiles, lev_count, LANES), jnp.float32),
            pltpu.VMEM((lev_count, LANES), jnp.float32),
            pltpu.SemaphoreType.DMA((4,)),
            pltpu.SemaphoreType.DMA((field_count, row_count)),
            pltpu.SemaphoreType.DMA((field_count, row_count + 1)),
        ],
        compiler_params=pltpu.CompilerParams(vmem_limit_bytes=START_LIMIT),
        cost_estimate=cost([part] * field_count, [part] * field_count, 3),
    )(departure_row, lat_fraction, lon_fraction, extents, fields)


def sums_kernel(row_count, *refs):
    parts, mine = refs[:-1], refs[-1]
    tile_count = parts[0].shape[0] // row_count
    at = lax.broadcasted_iota(jnp.int32, (1, LANES), 1)
    line = parts[0][row_count * tile_count][:1]
    for r in range(row_count):
        for f, part in enumerate(parts):
            tiles = [part[r * tile_count + n] for n in range(tile_count)]
            while len(tiles) > 1:
                tiles = [sum(tiles[k : k + 2]) for k in range(0, len(tiles), 2)]
            line = jnp.where(at == 3 * row_count + r * len(parts) + f, jnp.sum(tiles[0]), line)
    mine[...] = jnp.broadcast_to(line[None], mine.shape)


def exchange(parts, row_count):
    copies = lax.axis_size("lat") * lax.axis_size("lev")
    mine = pl.pallas_call(
        functools.partial(sums_kernel, row_count),
        out_shape=jax.ShapeDtypeStruct((copies, 1, LANES), jnp.float32),
        in_specs=[vmem()] * len(parts),
        out_specs=vmem(),
        compiler_params=pltpu.CompilerParams(vmem_limit_bytes=VMEM_LIMIT),
        cost_estimate=cost(parts, parts[:1], 3),
    )(*parts)
    return lax.all_to_all(mine, ("lat", "lev"), 0, 0, tiled=True)


def collect_kernel(*refs):
    parts, tiles, sems = refs[:-2], refs[-2], refs[-1]
    copies = [
        pltpu.make_async_copy(part.at[part.shape[0] - 1], tiles.at[k], sems.at[k])
        for k, part in enumerate(parts)
    ]
    for copy in copies:
        copy.start()
    for copy in copies:
        copy.wait()


def collect(parts):
    return pl.pallas_call(
        collect_kernel,
        out_shape=jax.ShapeDtypeStruct((len(parts),) + parts[0].shape[1:], jnp.float32),
        in_specs=[hbm()] * len(parts),
        out_specs=vmem(),
        scratch_shapes=[pltpu.SemaphoreType.DMA((len(parts),))],
        compiler_params=pltpu.CompilerParams(vmem_limit_bytes=VMEM_LIMIT),
        cost_estimate=pl.CostEstimate(flops=1000, bytes_accessed=8000, transcendentals=0),
    )(*parts)


def add_bands(plan, band_refs, band_ids, row_count, out_ref):
    tile_count = out_ref.shape[0] // row_count

    def row(r, carry):
        first = plan[0, r].astype(jnp.int32) - 1
        weights = cubic_weights(plan[0, row_count + r])
        for ref, band in zip(band_refs, band_ids):
            local = first - band * row_count

            @pl.when((local > -4) & (local < row_count))
            def _():
                total = out_ref[pl.ds(r * tile_count, tile_count)]
                for a in range(4):
                    index = local + a
                    inside = (index >= 0) & (index < row_count)
                    weight = jnp.where(inside, weights[a], 0.0)
                    index = jnp.clip(index, 0, row_count - 1)
                    total = total + weight * ref[pl.ds(index * tile_count, tile_count)]
                out_ref[pl.ds(r * tile_count, tile_count)] = total

        return carry

    lax.fori_loop(0, row_count, row, 0)


def combine_kernel(row_count, jobs, *refs):
    me = lax.axis_index("lat")
    outs = refs[len(refs) - len(jobs) :]
    for (bands, places, plan, line, seeds), out in zip(jobs, outs):
        span = pl.ds(0, out.shape[0])
        out[...] = sum((refs[seed][span] for seed in seeds[1:]), refs[seeds[0]][span]) if seeds else jnp.zeros_like(out)
        band_ids = [place(me) for place in places]
        add_bands(refs[plan].at[line(me)], [refs[b] for b in bands], band_ids, row_count, out)


def combine(row_count, *jobs):
    scalars, arrays = [], []

    def index(array, known):
        for k, other in enumerate(known):
            if other is array:
                return k
        known.append(array)
        return len(known) - 1

    kept = []
    for bands, places, (plan, line), *seeds in jobs:
        held = [index(b, arrays) for b in bands]
        kept.append((held, places, index(plan, scalars), line, [index(x, arrays) for x in seeds]))
    shift = len(scalars)
    kept = [
        ([b + shift for b in held], places, plan, line, [x + shift for x in seeds])
        for held, places, plan, line, seeds in kept
    ]
    tiles, lev_count, _ = jobs[0][0][0].shape
    outs = [jax.ShapeDtypeStruct((tiles - 1, lev_count, LANES), jnp.float32)] * len(jobs)
    return pl.pallas_call(
        functools.partial(combine_kernel, row_count, kept),
        out_shape=outs,
        in_specs=[smem()] * len(scalars) + [vmem()] * len(arrays),
        out_specs=[vmem()] * len(outs),
        compiler_params=pltpu.CompilerParams(vmem_limit_bytes=VMEM_LIMIT),
        cost_estimate=cost(arrays, outs, 8 * len(outs)),
    )(*scalars, *arrays)


def finish_kernel(split, plan, shifts, ratio, *refs):
    pieces = refs[: sum(len(held) for _, held in split)]
    out, kept, twice, ready, plan_s, shifts_s, ratio_s, scalar_sems, in_sems, sems = refs[-10:]
    row_count, lev_count, lon_count = ready.shape[1:]
    tile_count = lon_count // LANES
    group = twice.shape[0]
    lane = lax.broadcasted_iota(jnp.int32, (lev_count, LANES), 1)
    scalars = [
        pltpu.make_async_copy(source, target, scalar_sems.at[k])
        for k, (source, target) in enumerate(zip((plan, shifts, ratio), (plan_s, shifts_s, ratio_s)))
    ]

    def fetch(p, step):
        span = pl.ds(step * group * tile_count, group * tile_count)
        return pltpu.make_async_copy(pieces[p].at[span], kept.at[p, span], in_sems.at[p, step])

    for copy in scalars:
        copy.start()
    for _, held in split:
        for step in range(row_count // group):
            for p in held:
                fetch(p, step).start()
    for copy in scalars:
        copy.wait()

    for k, (field, held) in enumerate(split):

        def ship(r):
            return pltpu.make_async_copy(ready.at[k, r], out.at[r, field], sems.at[k, r])

        def rows(step, carry):
            for p in held:
                fetch(p, step).wait()
            for u in range(group):
                span = pl.ds((step * group + u) * tile_count, tile_count)
                column = kept[held[0], span]
                for p in held[1:]:
                    column = column + kept[p, span]
                twice[u, :tile_count] = column
                twice[u, tile_count : 2 * tile_count] = column
                twice[u, 2 * tile_count] = column[0]
            for u in range(group):
                r = step * group + u
                weights = cubic_weights(plan_s[0, 0, 2 * row_count + r])
                base = shifts_s[r] - 1
                base = jnp.where(base < 0, base + lon_count, base)
                moved = [None] * tile_count
                for tap in range(4):
                    first = (base + tap) // LANES
                    turn = (base + tap) % LANES
                    weight = weights[tap] * ratio_s[field]
                    keep = lane < LANES - turn
                    shift = jnp.where(turn == 0, 0, LANES - turn)
                    tiles = [pltpu.roll(twice[u, first + n], shift, axis=1) for n in range(tile_count + 1)]
                    for n in range(tile_count):
                        term = weight * jnp.where(keep, tiles[n], tiles[n + 1])
                        moved[n] = term if tap == 0 else moved[n] + term
                for n in range(tile_count):
                    ready[k, r, :, n * LANES : (n + 1) * LANES] = moved[n]

            @pl.when(step > 0)
            def _():
                for u in range(group):
                    ship((step - 1) * group + u).start()

            return carry

        lax.fori_loop(0, row_count // group, rows, 0)
        for u in range(group):
            ship(row_count - group + u).start()
    for k, (field, _) in enumerate(split):
        for r in range(row_count):
            pltpu.make_async_copy(ready.at[k, r], out.at[r, field], sems.at[k, r]).wait()


def finish(plan, shifts, ratio, pieces, out_shape, out=None):
    row_count, _, lev_count, lon_count = out_shape
    given = [] if out is None else [out]
    group = row_count
    flat, split = [], []
    for field, parts in pieces.items():
        split.append((field, tuple(range(len(flat), len(flat) + len(parts)))))
        flat += parts
    return pl.pallas_call(
        functools.partial(finish_kernel, split),
        out_shape=jax.ShapeDtypeStruct(out_shape, jnp.float32),
        in_specs=[hbm()] * (3 + len(flat) + len(given)),
        out_specs=hbm(),
        input_output_aliases={3 + len(flat): 0} if given else {},
        scratch_shapes=[
            pltpu.VMEM((len(flat),) + flat[0].shape, jnp.float32),
            pltpu.VMEM((group, 2 * lon_count // LANES + 1, lev_count, LANES), jnp.float32),
            pltpu.VMEM((len(split), row_count, lev_count, lon_count), jnp.float32),
            pltpu.SMEM(plan.shape, plan.dtype),
            pltpu.SMEM(shifts.shape, shifts.dtype),
            pltpu.SMEM(ratio.shape, ratio.dtype),
            pltpu.SemaphoreType.DMA((3,)),
            pltpu.SemaphoreType.DMA((len(flat), row_count // group)),
            pltpu.SemaphoreType.DMA((len(split), row_count)),
        ],
        compiler_params=pltpu.CompilerParams(vmem_limit_bytes=VMEM_LIMIT),
        cost_estimate=cost(flat, flat[:1], 60 * len(split)),
    )(plan, shifts, ratio, *flat, *given)


def mass_ratio(table, row_count, field_count):
    band_count, lev_size = lax.axis_size("lat"), lax.axis_size("lev")
    total_rows = band_count * row_count
    parts = table.reshape(band_count, lev_size, -1)
    columns = [parts[:, 0, k * row_count : (k + 1) * row_count].reshape(total_rows) for k in range(3)]
    first = columns[0].astype(jnp.int32) - 1
    lat_w = cubic_weights(columns[1])
    lon_w = cubic_weights(columns[2])
    sums = parts[:, :, 3 * row_count : (3 + field_count) * row_count].sum(1).reshape(total_rows, field_count)
    row_ids = jnp.arange(total_rows, dtype=jnp.int32)
    area = jnp.cos(math.pi * (row_ids.astype(jnp.float32) + 0.5) / total_rows - math.pi / 2.0)
    gain = area * (lon_w[0] + lon_w[1] + lon_w[2] + lon_w[3])
    hit = jnp.zeros((total_rows, total_rows), jnp.float32)
    for a in range(4):
        hit = hit + jnp.where((first + a)[:, None] == row_ids[None, :], (gain * lat_w[a])[:, None], 0.0)
    after_w = hit.sum(0)
    before = (area[:, None] * sums).sum(0)
    after = (after_w[:, None] * sums).sum(0)
    return before / after


def one_step(fields, lat_fraction, lon_fraction, lon_shift, departure_row, extents):
    row_count, field_count = fields.shape[:2]
    near, middle, both = flip(1), flip(2), flip(3)
    even, odd = flip(REACH), across
    join = functools.partial(combine, row_count)
    scalars = departure_row, lat_fraction, lon_fraction, extents
    f2, f0, plan = start((2, 0), *scalars, fields)
    f1, _ = start((1,), *scalars, fields)
    both_plan = send(plan, both)
    f2_middle = send(f2, middle)
    f0_even = send(f0, even)
    f0_odd = send(f0, odd)
    f1_near = send(f1, near)
    f1_middle = send(f1, middle)
    table = exchange([from_hbm(f) for f in (f0, f1, f2)], row_count)
    f2_even = send(f2, even)
    f2_odd = send(f2, odd)
    f1_both = send(f1_near, middle)
    f2_side = send(f2_middle, onward)

    f0, f1, f2 = (from_hbm(f) for f in (f0, f1, f2))
    plans = collect([f1_near, f2_middle, f0_even, f0_odd])
    near_plan, middle_plan = (plans, lambda me: 0), (plans, lambda me: 1)
    onward_plan = (plans, lambda me: jnp.where(onward(me) == even(me), 2, 3))
    back_plan = (plans, lambda me: jnp.where(back(me) == even(me), 2, 3))
    own_plan, far_plan = (plan, lambda me: 0), (both_plan, lambda me: 0)

    f0_all = [f0, f0_even, f0_odd], [stay, even, odd]
    (for_both,) = join((*f0_all, far_plan))
    f0_relay = send(for_both, near)
    (for_near,) = join((*f0_all, near_plan))
    f0_from_near = send(for_near, near)
    (for_middle,) = join((*f0_all, middle_plan, f0_relay))
    f0_from_middle = send(for_middle, middle)

    (for_back,) = join(([f1, f1_near], [stay, near], back_plan))
    f1_from_onward = send(for_back, back)
    f1_all = [f1, f1_near, f1_middle], [stay, near, middle]
    f1_early, f1_own = join((*f1_all, onward_plan), (*f1_all, own_plan))
    f2_all = [f2, f2_middle, f2_even, f2_odd], [stay, middle, even, odd]
    f2_early, f2_own = join((*f2_all, near_plan), (*f2_all, own_plan))
    (for_onward,) = join(([f1_both], [both], onward_plan, f1_early))
    f1_from_back = send(for_onward, onward)
    (f2_for_near,) = join(([f2_side], [side], near_plan, f2_early))
    f2_from_near = send(f2_for_near, near)
    (f0_own,) = join((*f0_all, own_plan, f0_from_near))
    (f1_own,) = join(([f1_both], [both], own_plan, f1_own, f1_from_onward))
    (f2_own,) = join(([f2_side], [side], own_plan, f2_own))

    ratio = mass_ratio(table, row_count, field_count)
    pieces = [f0_own, f0_from_middle], [f1_own, f1_from_back], [f2_own, f2_from_near]
    out = None
    for field, parts in enumerate(pieces):
        out = finish(plan, lon_shift, ratio, {field: parts}, fields.shape, out)
    return out


def solution(mesh):
    return jax.shard_map(
        one_step,
        mesh=mesh,
        in_specs=(
            P("lat", None, "lev", None),
            P("lat"),
            P("lat"),
            P("lat"),
            P("lat"),
            P("lat", None),
        ),
        out_specs=P("lat", None, "lev", None),
        check_vma=False,
    )
```
